32 devices in a mesh: grp: 2 (over y), seq: 16 (over z, x, core).
Axes of the slice: x: 2, y: 2, z: 4, core: 2. Of those that a mesh axis runs over, the one named last changes fastest.
Arguments:
- frames: bfloat16 [4, 10240, 1280], P('grp', 'seq'), parts along dimension 0, may hold values from -120 to 120
- dec_states: bfloat16 [2, 256, 1280], P(None, 'grp'), parts along dimension 1, may hold values from -6 to 6
- w_query: bfloat16 [1280, 1280], P(None, 'seq'), may hold values from -0.15625 to 0.15625
- w_keyval: bfloat16 [1280, 2560], replicated, may hold values from -0.15625 to 0.15625
- w_output: bfloat16 [1280, 1280], P(None, 'seq'), may hold values from -0.15625 to 0.15625
- head_slope: float32 [20], replicated, may hold values from 0.3 to 12
- lengths: int32 [4, 16], P('grp'), parts along dimension 0, may hold values from 128 to 640, as said below
- positions: int32 [2, 256], P(None, 'grp'), parts along dimension 1, may hold values from 0 to 15
Outputs:
- attended: bfloat16 [2, 256, 1280], P(None, 'grp', 'seq'), parts along dimension 1
The draws below stay inside these ranges and needn't reach their ends.
There are 2 independent parts, one for each index of `grp`. The reference program is written for one: setup_inputs(seed, part) draws one part's arguments, and reference() takes and returns one part's arrays. A program takes and returns all parts, laid end to end along the dimension named above; an argument that names none is the same for every part. Nothing has to cross between parts.
Inputs may be any that keep to these rules, and one draw needn't show every extreme that they name: `lengths`: every step has one block of exactly 640 valid frames.
All inputs are finite; a program needn't handle non-finite values.
Results may differ from the reference program's by a relative error of at most 0.005.
The reference program's roundings to bfloat16 on the way count: a program that leaves them out, or rounds other values in their place, can miss the bound.
Values may be sent and summed in bfloat16 or wider, within the bound.
A program may use at most 128 MiB of HBM per device.

```python
import math
import jax
import jax.numpy as jnp
from jax import lax

D = 1280
H = 20
FR = 640
STEPS = 2
QROWS = 128
N_SEQ = 16


def draw_frames(key, part):
    key_base = jax.random.fold_in(key, 11)
    base = jax.random.normal(key_base, (STEPS, N_SEQ * FR, D), jnp.float32)
    base = jnp.clip(base, -6.0, 6.0)
    return base.astype(jnp.bfloat16)


def draw_lengths(key, part):
    key_pick = jax.random.fold_in(key, 21)
    key_long = jax.random.fold_in(key, 22)
    lowest = FR // 5
    spread = FR - lowest
    picked = jax.random.randint(key_pick, (STEPS, N_SEQ), 0, spread + 1)
    frame_counts = lowest + picked * picked // spread
    longest = jax.random.randint(key_long, (STEPS,), 0, N_SEQ)
    longest_at = jnp.arange(N_SEQ, dtype=jnp.int32)[None, :] == longest[:, None]
    return jnp.where(longest_at, FR, frame_counts).astype(jnp.int32)


def plant(values, own_key, smallest, high):
    spot = [jax.random.randint(jax.random.fold_in(own_key, axis), (), 0, length) for axis, length in enumerate(values.shape)]
    main_axis = values.shape.index(max(values.shape))
    neighbour = spot[:main_axis] + [(spot[main_axis] + 1) % values.shape[main_axis]] + spot[main_axis + 1:]
    return values.at[tuple(spot)].set(smallest).at[tuple(neighbour)].set(high)


def block_levels(own_key, extent, split, least, largest):
    level, own = 1.0, jax.random.fold_in(own_key, 6)
    for axis_at, shards_of in split:
        draws = jnp.exp(jax.random.uniform(jax.random.fold_in(own, axis_at), (shards_of,), jnp.float32, least / len(split), largest / len(split)))
        level = level * jnp.repeat(draws, extent[axis_at] // shards_of).reshape([-1 if axis == axis_at else 1 for axis in range(len(extent))])
    return level


def noise(rng, shape, scale, most, pieces=(), kind=jnp.bfloat16):
    result = jax.random.normal(rng, shape, jnp.float32) * scale
    if len(pieces) > 0:
        result = block_levels(rng, shape, pieces, -0.22, 0.18) * result
    return jnp.clip(result, min=-most, max=most).astype(kind)


def setup_inputs(seed: int = 0, part: int = 0) -> dict:
    splits = jax.random.split(jax.random.key(seed), 9)
    part_splits = jax.random.split(jax.random.fold_in(splits[8], part), 9)
    return {
        "frames": draw_frames(jax.random.fold_in(jax.random.fold_in(splits[8], part), 71), part),
        "dec_states": noise(part_splits[1], (STEPS, QROWS, D), 1.0, 6.0),
        "w_query": noise(splits[2], (D, D), D ** -0.5, 0.15625, ((1, 16),)),
        "w_keyval": noise(splits[3], (D, 2 * D), D ** -0.5, 0.15625),
        "w_output": noise(splits[4], (D, D), D ** -0.5, 0.15625, ((1, 16),)),
        "head_slope": jnp.clip(jnp.exp(jax.random.uniform(splits[5], (H,), jnp.float32, math.log(0.3), math.log(12.0))), 0.3, 12.0),
        "lengths": draw_lengths(jax.random.fold_in(jax.random.fold_in(splits[8], part), 71), part),
        "positions": plant(jax.random.randint(part_splits[7], (STEPS, QROWS), 0, N_SEQ), jax.random.fold_in(part_splits[7], 1), 0, N_SEQ - 1).astype(jnp.int32),
    }


def reference(frames, dec_states, w_query, w_keyval, w_output, head_slope, lengths, positions):
    step_count, total_frames, model_width = frames.shape
    query_rows = dec_states.shape[1]
    head_count = head_slope.shape[0]
    head_size = model_width // head_count
    block_count = N_SEQ
    frame_count = total_frames // block_count
    keyval = jnp.dot(frames.reshape(step_count * total_frames, model_width), w_keyval, preferred_element_type=jnp.float32).astype(jnp.bfloat16)
    all_keys = keyval[:, :model_width].reshape(step_count, block_count, frame_count, head_count, head_size)
    all_values = keyval[:, model_width:].reshape(step_count, block_count, frame_count, head_count, head_size)
    queries = jnp.dot(dec_states.reshape(step_count * query_rows, model_width), w_query, preferred_element_type=jnp.float32).astype(jnp.bfloat16)
    queries = queries.reshape(step_count, query_rows, head_count, head_size)
    results = []
    for step_now in range(step_count):
        query_now = queries[step_now].astype(jnp.float32)
        row_positions = positions[step_now].astype(jnp.float32)

        def one_block(flat_index):
            older_step = flat_index // block_count
            block_index = flat_index % block_count
            block_keys = all_keys[older_step, block_index].astype(jnp.float32)
            block_values = all_values[older_step, block_index].astype(jnp.float32)
            scores = jnp.einsum('qhd,jhd->hqj', query_now, block_keys) / math.sqrt(head_size)
            slot_place = ((block_index + 1) % block_count).astype(jnp.float32)
            age_steps = (step_now - older_step).astype(jnp.float32)
            distance = jnp.abs(row_positions - slot_place) / block_count + age_steps
            scores = scores - head_slope[:, None, None] * distance[None, :, None]
            length_now = lengths[older_step, block_index]
            valid = jnp.arange(frame_count, dtype=jnp.int32)[None, None, :] < length_now
            scores = jnp.where(valid, scores, -jnp.inf)
            row_peak = lax.optimization_barrier(jnp.max(scores, axis=2))
            weights = jnp.exp(scores - row_peak[:, :, None]).astype(jnp.bfloat16).astype(jnp.float32)
            row_total = lax.optimization_barrier(jnp.sum(weights, axis=2))
            row_context = jnp.einsum('hqj,jhd->hqd', weights, block_values)
            return (row_peak, row_total, row_context)
        peaks, totals, contexts = lax.map(one_block, jnp.arange((step_now + 1) * block_count, dtype=jnp.int32))
        row_top = lax.optimization_barrier(jnp.max(peaks, axis=0))
        factors = jnp.exp(peaks - row_top[None])
        row_total = lax.optimization_barrier(jnp.sum(factors * totals, axis=0))
        row_context = lax.optimization_barrier(jnp.sum(factors[..., None] * contexts, axis=0))
        context = (row_context / row_total[..., None]).transpose(1, 0, 2).reshape(query_rows, model_width)
        context = context.astype(jnp.bfloat16)
        results.append(jnp.dot(context, w_output, preferred_element_type=jnp.float32).astype(jnp.bfloat16))
    return jnp.stack(results)
```

```python
import functools
import math

import jax
import jax.numpy as jnp
from jax import lax
from jax.experimental import pallas as pl
from jax.experimental.pallas import tpu as pltpu
from jax.sharding import PartitionSpec as P

MESH = pl.DeviceIdType.MESH
EXTRA = 16
MASKED = -1e30


def rows_together(ref, first, count):
    parts = [ref[first + index].astype(jnp.float32) for index in range(count)]
    return jnp.concatenate(parts, axis=0)


def await_bytes(ref, count, sem):
    part = ref.at[pl.ds(0, count)]
    pltpu.make_async_copy(part, part, sem).wait()


def kernel(
    n,
    dec_ref,
    wq_ref,
    wout_ref,
    pos_ref,
    slope_ref,
    len_ref,
    frames_hbm,
    wkv_hbm,
    out_ref,
    frames_ref,
    wkv_ref,
    k_ref,
    vt_ref,
    q_ref,
    ctx_ref,
    stat_ref,
    got_ctx,
    got_stat,
    fin_ref,
    frame_sem,
    weight_sem,
    send_sem,
    recv_sem,
):
    me = lax.axis_index("seq")
    steps, frame_count, width = frames_hbm.shape
    tokens = dec_ref.shape[0]
    per_step = tokens // steps
    heads = k_ref.shape[0]
    size = width // heads
    rows = wq_ref.shape[1]
    groups = math.gcd(heads, n)
    group_chunks = n // groups
    group_heads = heads // groups
    tile = frames_ref.shape[1]
    half = wkv_ref.shape[2]
    tiles = frames_ref.shape[0]
    per_block = frame_count // tile
    scale = 1.0 / math.sqrt(size)

    def frame_copy(index):
        return pltpu.make_async_copy(
            frames_hbm.at[index // per_block, pl.ds((index % per_block) * tile, tile)],
            frames_ref.at[index],
            frame_sem.at[index],
        )

    def weight_copy(index):
        return pltpu.make_async_copy(
            wkv_hbm.at[:, pl.ds(index * half, half)], wkv_ref.at[index], weight_sem.at[index]
        )

    frame_copy(0).start()
    weight_copy(0).start()
    for index in range(1, tiles):
        frame_copy(index).start()
    for index in range(1, wkv_ref.shape[0]):
        weight_copy(index).start()

    barrier = pltpu.get_barrier_semaphore()

    @pl.loop(1, n)
    def _(step):
        peer = lax.rem(me + step, n)
        pl.semaphore_signal(barrier, inc=1, device_id={"seq": peer}, device_id_type=MESH)

    own_query = jnp.dot(dec_ref[...], wq_ref[...], preferred_element_type=jnp.float32)
    q_ref[me] = own_query.T.astype(jnp.bfloat16)
    pl.semaphore_wait(barrier, n - 1)

    def send(src, dst, sem, peer):
        pltpu.make_async_remote_copy(
            src_ref=src,
            dst_ref=dst,
            send_sem=send_sem.at[sem],
            recv_sem=recv_sem.at[sem],
            device_id={"seq": peer},
            device_id_type=MESH,
        ).start()

    @pl.loop(1, n)
    def _(step):
        send(q_ref.at[me], q_ref.at[me], 0, lax.rem(me + step, n))

    column = lax.broadcasted_iota(jnp.int32, (frame_count, EXTRA), 1)
    place = lax.broadcasted_iota(jnp.int32, (frame_count, EXTRA), 0)
    masks = []
    for older in range(steps):
        hidden = (place >= len_ref[older, me]) & (column == 0)
        masks.append(jnp.where(hidden, MASKED, 0.0).astype(jnp.bfloat16))
    mask = jnp.concatenate(masks, axis=0)
    ones = jnp.ones((EXTRA, steps * frame_count), jnp.bfloat16)

    @pl.loop(0, heads)
    def _(head):
        k_ref[head, :, size:] = mask
        vt_ref[head, size:, :] = ones

    halves = wkv_ref.shape[0]
    half_heads = half // size
    for part in range(halves):
        weight_copy(part).wait()

        @pl.loop(0, tiles)
        def _(index):
            if part == 0:
                frame_copy(index).wait()
            keyval = jnp.dot(
                frames_ref[index], wkv_ref[part], preferred_element_type=jnp.float32
            )
            at = pl.ds(pl.multiple_of(index * tile, tile), tile)
            if part < halves // 2:
                keyval = keyval.astype(jnp.bfloat16)
                for local_head in range(half_heads):
                    head = part * half_heads + local_head
                    k_ref[head, at, 0:size] = keyval[:, local_head * size : (local_head + 1) * size]
            else:
                turned = keyval.T.astype(jnp.bfloat16)
                for local_head in range(half_heads):
                    head = (part - halves // 2) * half_heads + local_head
                    vt_ref[head, 0:size, at] = turned[local_head * size : (local_head + 1) * size]

    await_bytes(q_ref, n - 1, send_sem.at[0])
    await_bytes(q_ref, n - 1, recv_sem.at[0])

    slot_place = lax.rem(me + 1, n).astype(jnp.float32)
    distance = jnp.abs(pos_ref[...].astype(jnp.float32) - slot_place) / n
    first_row = lax.broadcasted_iota(jnp.int32, (EXTRA, tokens), 0) == 0
    query_tail = jnp.where(first_row, 1.0, 0.0).astype(jnp.bfloat16)
    token_step = lax.broadcasted_iota(jnp.int32, (1, tokens), 1) // per_step

    @pl.loop(0, groups)
    def _(turn):
        group = lax.rem(me // group_chunks + 1 + turn, groups)
        query_rows = rows_together(q_ref, group * group_chunks, group_chunks).astype(jnp.bfloat16)
        peaks, totals, contexts = [], [], []
        for local_head in range(group_heads):
            head = group * group_heads + local_head
            query = jnp.concatenate(
                [query_rows[local_head * size : (local_head + 1) * size], query_tail], axis=0
            )
            slope = slope_ref[head]
            peak = context = None
            for older in range(steps):
                first = older * per_step
                block = pl.ds(older * frame_count, frame_count)
                raw = jnp.dot(
                    k_ref[head, block, :], query[:, first:], preferred_element_type=jnp.float32
                )
                raw_peak = jnp.max(raw, axis=0, keepdims=True)
                weights = jnp.exp2((raw - raw_peak) * (scale * math.log2(math.e)))
                part_context = jnp.dot(
                    vt_ref[head, :, block],
                    weights.astype(jnp.bfloat16),
                    preferred_element_type=jnp.float32,
                )
                age = (token_step[:, first:] - older).astype(jnp.float32)
                part_peak = raw_peak * scale - slope * (distance[:, first:] + age)
                if peak is None:
                    peak, context = part_peak, part_context
                    continue
                top = jnp.maximum(peak[:, first:], part_peak)
                old_factor = jnp.exp(peak[:, first:] - top)
                new_factor = jnp.exp(part_peak - top)
                merged = context[:, first:] * old_factor + part_context * new_factor
                peak = jnp.concatenate([peak[:, :first], top], axis=1)
                context = jnp.concatenate([context[:, :first], merged], axis=1)
            peaks.append(peak)
            totals.append(context[size : size + 1])
            contexts.append(context[:size])
        stacked = jnp.concatenate(contexts, axis=0)
        for index in range(group_chunks):
            low, high = index * rows, (index + 1) * rows
            one, two = low // size, (high - 1) // size
            chunk = group * group_chunks + index
            ctx_ref[chunk] = stacked[low:high].astype(jnp.bfloat16)
            stat_ref[chunk] = jnp.concatenate(
                [peaks[one], peaks[two], totals[one], totals[two]], axis=0
            )

        @pl.loop(0, group_chunks)
        def _(index):
            chunk = group * group_chunks + lax.rem(me + index, group_chunks)

            @pl.when(chunk != me)
            def _():
                send(stat_ref.at[chunk], got_stat.at[me], 1, chunk)
                send(ctx_ref.at[chunk], got_ctx.at[me], 2, chunk)

    got_stat[me] = stat_ref[me]
    got_ctx[me] = ctx_ref[me]
    await_bytes(got_stat, n - 1, recv_sem.at[1])
    await_bytes(got_ctx, n - 1, recv_sem.at[2])
    await_bytes(stat_ref, n - 1, send_sem.at[1])
    await_bytes(ctx_ref, n - 1, send_sem.at[2])

    top = lax.fori_loop(
        1, n, lambda at, best: jnp.maximum(best, got_stat[at][0:2]), got_stat[0][0:2]
    )
    row = lax.broadcasted_iota(jnp.int32, (rows, tokens), 0)
    is_one = row + lax.rem(me * rows, size) < size

    def add(at, state):
        total, acc = state
        stat = got_stat[at]
        factor = jnp.exp(stat[0:2] - top)
        spread = jnp.where(is_one, factor[0:1], factor[1:2])
        return total + stat[2:4] * factor, acc + got_ctx[at].astype(jnp.float32) * spread

    total, acc = lax.fori_loop(
        0,
        n,
        add,
        (jnp.zeros((2, tokens), jnp.float32), jnp.zeros((rows, tokens), jnp.float32)),
    )
    fin_ref[me] = (acc / jnp.where(is_one, total[0:1], total[1:2])).astype(jnp.bfloat16)

    @pl.loop(1, n)
    def _(step):
        send(fin_ref.at[me], fin_ref.at[me], 3, lax.rem(me + step, n))

    await_bytes(fin_ref, n - 1, recv_sem.at[3])
    await_bytes(fin_ref, n - 1, send_sem.at[3])
    turned = rows_together(fin_ref, 0, n).T.astype(jnp.bfloat16)
    attended = jnp.dot(turned, wout_ref[...], preferred_element_type=jnp.float32)
    out_ref[...] = attended.astype(jnp.bfloat16)


def local(n, frames, dec_states, w_query, w_keyval, w_output, head_slope, lengths, positions):
    steps, frame_count, width = frames.shape
    per_step = dec_states.shape[1]
    tokens = steps * per_step
    heads = head_slope.shape[0]
    size = width // heads
    rows = w_query.shape[1]
    keys = steps * frame_count
    tile = math.gcd(frame_count, 128)
    half = width // 2
    vmem = pl.BlockSpec(memory_space=pltpu.VMEM)
    smem = pl.BlockSpec(memory_space=pltpu.SMEM)
    hbm = pl.BlockSpec(memory_space=pl.ANY)
    out = pl.pallas_call(
        functools.partial(kernel, n),
        out_shape=jax.ShapeDtypeStruct((tokens, rows), jnp.bfloat16),
        in_specs=[vmem, vmem, vmem, vmem, smem, smem, hbm, hbm],
        out_specs=vmem,
        scratch_shapes=[
            pltpu.VMEM((keys // tile, tile, width), jnp.bfloat16),
            pltpu.VMEM((4, width, half), jnp.bfloat16),
            pltpu.VMEM((heads, keys, size + EXTRA), jnp.bfloat16),
            pltpu.VMEM((heads, size + EXTRA, keys), jnp.bfloat16),
            pltpu.VMEM((n, rows, tokens), jnp.bfloat16),
            pltpu.VMEM((n, rows, tokens), jnp.bfloat16),
            pltpu.VMEM((n, 4, tokens), jnp.float32),
            pltpu.VMEM((n, rows, tokens), jnp.bfloat16),
            pltpu.VMEM((n, 4, tokens), jnp.float32),
            pltpu.VMEM((n, rows, tokens), jnp.bfloat16),
            pltpu.SemaphoreType.DMA((keys // tile,)),
            pltpu.SemaphoreType.DMA((4,)),
            pltpu.SemaphoreType.DMA((4,)),
            pltpu.SemaphoreType.DMA((4,)),
        ],
        compiler_params=pltpu.CompilerParams(
            collective_id=0, has_side_effects=True, vmem_limit_bytes=60 * 1024 * 1024
        ),
    )(
        dec_states.reshape(tokens, width),
        w_query,
        w_output,
        positions.reshape(1, tokens),
        head_slope,
        lengths,
        frames,
        w_keyval,
    )
    return out.reshape(steps, per_step, rows)


def solution(mesh):
    return jax.shard_map(
        functools.partial(local, mesh.shape["seq"]),
        mesh=mesh,
        in_specs=(
            P("grp", "seq", None),
            P(None, "grp", None),
            P(None, "seq"),
            P(),
            P(None, "seq"),
            P(),
            P("grp", None),
            P(None, "grp"),
        ),
        out_specs=P(None, "grp", "seq"),
        check_vma=False,
    )
```

```python
import functools
import math

import jax
import jax.numpy as jnp
from jax import lax
from jax.experimental import pallas as pl
from jax.experimental.pallas import tpu as pltpu
from jax.sharding import PartitionSpec as P

MESH = pl.DeviceIdType.MESH
EXTRA = 16
MASKED = -1e30


def rows_together(ref, first, count):
    parts = [ref[first + index].astype(jnp.float32) for index in range(count)]
    return jnp.concatenate(parts, axis=0)


def await_bytes(ref, count, sem):
    part = ref.at[pl.ds(0, count)]
    pltpu.make_async_copy(part, part, sem).wait()


def kernel(
    n,
    dec_ref,
    wq_ref,
    wout_ref,
    pos_ref,
    slope_ref,
    len_ref,
    frames_hbm,
    wkv_hbm,
    out_ref,
    frames_ref,
    wkv_ref,
    k_ref,
    vt_ref,
    q_ref,
    ctx_ref,
    stat_ref,
    got_ctx,
    got_stat,
    fin_ref,
    frame_sem,
    weight_sem,
    send_sem,
    recv_sem,
    hop_sem,
):
    me = lax.axis_index("seq")
    steps, frame_count, width = frames_hbm.shape
    tokens = dec_ref.shape[0]
    per_step = tokens // steps
    heads = k_ref.shape[0]
    size = width // heads
    rows = wq_ref.shape[0]
    groups = math.gcd(heads, n)
    group_chunks = n // groups
    group_heads = heads // groups
    tile = frames_ref.shape[1]
    half = wkv_ref.shape[2]
    tiles = frames_ref.shape[0]
    per_block = frame_count // tile
    scale = 1.0 / math.sqrt(size)

    def frame_copy(index):
        return pltpu.make_async_copy(
            frames_hbm.at[index // per_block, pl.ds((index % per_block) * tile, tile)],
            frames_ref.at[index],
            frame_sem.at[index],
        )

    def weight_copy(index):
        return pltpu.make_async_copy(
            wkv_hbm.at[:, pl.ds(pl.multiple_of(index * half, half), half)], wkv_ref.at[index], weight_sem.at[index]
        )

    frame_copy(0).start()
    weight_copy(0).start()
    for index in range(1, tiles):
        frame_copy(index).start()
    for index in range(1, wkv_ref.shape[0]):
        weight_copy(index).start()

    barrier = pltpu.get_barrier_semaphore()

    @pl.loop(1, n)
    def _(step):
        peer = lax.rem(me + step, n)
        pl.semaphore_signal(barrier, inc=1, device_id={"seq": peer}, device_id_type=MESH)

    own_query = lax.dot_general(
        wq_ref[...], dec_ref[...], (((1,), (1,)), ((), ())), preferred_element_type=jnp.float32
    )
    q_ref[me] = own_query.astype(jnp.bfloat16)
    pl.semaphore_wait(barrier, n - 1)

    def send(src, dst, sem, peer):
        pltpu.make_async_remote_copy(
            src_ref=src,
            dst_ref=dst,
            send_sem=send_sem.at[sem],
            recv_sem=recv_sem.at[sem],
            device_id={"seq": peer},
            device_id_type=MESH,
        ).start()

    @pl.loop(1, n)
    def _(step):
        send(q_ref.at[me], q_ref.at[me], 0, lax.rem(me + step, n))

    column = lax.broadcasted_iota(jnp.int32, (frame_count, size + EXTRA), 1)
    place = lax.broadcasted_iota(jnp.int32, (frame_count, size + EXTRA), 0)
    masks = []
    for older in range(steps):
        hidden = (place >= len_ref[older, me]) & (column == size)
        masks.append(jnp.where(hidden, MASKED, 0.0).astype(jnp.bfloat16))
    mask = jnp.concatenate(masks, axis=0)
    ones = jnp.ones((EXTRA, steps * frame_count), jnp.bfloat16)

    @pl.loop(0, heads)
    def _(head):
        k_ref[head] = mask
        vt_ref[head, size:, :] = ones

    parts = wkv_ref.shape[0] // 2
    part_heads = half // size

    def project(part, index):
        at = pl.ds(pl.multiple_of(index * tile, tile), tile)
        keyval = jnp.dot(frames_ref[index], wkv_ref[part], preferred_element_type=jnp.float32)
        return at, keyval.astype(jnp.bfloat16)

    for index in range(tiles):
        frame_copy(index).wait()

    @pl.loop(0, parts)
    def _(part):
        weight_copy(part).wait()
        for index in range(tiles):
            at, keyval = project(part, index)
            for local_head in range(part_heads):
                lanes = slice(local_head * size, (local_head + 1) * size)
                k_ref[part * part_heads + local_head, at, 0:size] = keyval[:, lanes]

    @pl.loop(0, parts)
    def _(part):
        weight_copy(parts + part).wait()
        for index in range(tiles):
            at, keyval = project(parts + part, index)
            turned = keyval.T
            for local_head in range(part_heads):
                lanes = slice(local_head * size, (local_head + 1) * size)
                vt_ref[part * part_heads + local_head, 0:size, at] = turned[lanes]

    await_bytes(q_ref, n - 1, send_sem.at[0])
    await_bytes(q_ref, n - 1, recv_sem.at[0])

    slot_place = lax.rem(me + 1, n).astype(jnp.float32)
    distance = jnp.abs(pos_ref[...].astype(jnp.float32) - slot_place) / n
    first_row = lax.broadcasted_iota(jnp.int32, (EXTRA, tokens), 0) == 0
    query_tail = jnp.where(first_row, 1.0, 0.0).astype(jnp.bfloat16)
    token_step = lax.broadcasted_iota(jnp.int32, (1, tokens), 1) // per_step

    @pl.loop(0, groups)
    def _(turn):
        group = lax.rem(me // group_chunks + 1 + turn, groups)
        query_rows = rows_together(q_ref, group * group_chunks, group_chunks).astype(jnp.bfloat16)
        peaks, totals, contexts = [], [], []
        for local_head in range(group_heads):
            head = group * group_heads + local_head
            query = jnp.concatenate(
                [query_rows[local_head * size : (local_head + 1) * size], query_tail], axis=0
            )
            slope = slope_ref[head]
            peak = context = None
            for older in range(steps):
                first = older * per_step
                block = pl.ds(older * frame_count, frame_count)
                raw = jnp.dot(
                    k_ref[head, block, :], query[:, first:], preferred_element_type=jnp.float32
                )
                raw_peak = jnp.max(raw, axis=0, keepdims=True)
                weights = jnp.exp2((raw - raw_peak) * (scale * math.log2(math.e)))
                part_context = jnp.dot(
                    vt_ref[head, :, block],
                    weights.astype(jnp.bfloat16),
                    preferred_element_type=jnp.float32,
                )
                age = (token_step[:, first:] - older).astype(jnp.float32)
                part_peak = raw_peak * scale - slope * (distance[:, first:] + age)
                if peak is None:
                    peak, context = part_peak, part_context
                    continue
                top = jnp.maximum(peak[:, first:], part_peak)
                old_factor = jnp.exp(peak[:, first:] - top)
                new_factor = jnp.exp(part_peak - top)
                merged = context[:, first:] * old_factor + part_context * new_factor
                peak = jnp.concatenate([peak[:, :first], top], axis=1)
                context = jnp.concatenate([context[:, :first], merged], axis=1)
            peaks.append(peak)
            totals.append(context[size : size + 1])
            contexts.append(context[:size])
        stacked = jnp.concatenate(contexts, axis=0)
        for index in range(group_chunks):
            low, high = index * rows, (index + 1) * rows
            one, two = low // size, (high - 1) // size
            chunk = group * group_chunks + index
            ctx_ref[chunk] = stacked[low:high].astype(jnp.bfloat16)
            stat_ref[chunk] = jnp.concatenate(
                [peaks[one], peaks[two], totals[one], totals[two]], axis=0
            )

        @pl.loop(0, group_chunks)
        def _(index):
            chunk = group * group_chunks + lax.rem(me + index, group_chunks)

            @pl.when(chunk != me)
            def _():
                send(stat_ref.at[chunk], got_stat.at[me], 1, chunk)
                send(ctx_ref.at[chunk], got_ctx.at[me], 2, chunk)

    got_stat[me] = stat_ref[me]
    got_ctx[me] = ctx_ref[me]
    await_bytes(got_stat, n - 1, recv_sem.at[1])
    await_bytes(got_ctx, n - 1, recv_sem.at[2])
    await_bytes(stat_ref, n - 1, send_sem.at[1])
    await_bytes(ctx_ref, n - 1, send_sem.at[2])

    top = lax.fori_loop(
        1, n, lambda at, best: jnp.maximum(best, got_stat[at][0:2]), got_stat[0][0:2]
    )
    row = lax.broadcasted_iota(jnp.int32, (rows, tokens), 0)
    is_one = row + lax.rem(me * rows, size) < size

    def add(at, state):
        total, acc = state
        stat = got_stat[at]
        factor = jnp.exp(stat[0:2] - top)
        spread = jnp.where(is_one, factor[0:1], factor[1:2])
        return total + stat[2:4] * factor, acc + got_ctx[at].astype(jnp.float32) * spread

    total, acc = lax.fori_loop(
        0,
        n,
        add,
        (jnp.zeros((2, tokens), jnp.float32), jnp.zeros((rows, tokens), jnp.float32)),
    )
    fin_ref[me] = (acc / jnp.where(is_one, total[0:1], total[1:2])).astype(jnp.bfloat16)

    partner = me + 1 - 2 * lax.rem(me, 2)
    chips = n // 2

    def pass_on(chunk):
        pltpu.make_async_remote_copy(
            src_ref=fin_ref.at[chunk],
            dst_ref=fin_ref.at[chunk],
            send_sem=send_sem.at[3],
            recv_sem=recv_sem.at[3],
            device_id={"seq": partner},
            device_id_type=MESH,
        ).start()

    def hop(step):
        return pltpu.make_async_remote_copy(
            src_ref=fin_ref.at[me],
            dst_ref=fin_ref.at[me],
            send_sem=send_sem.at[0],
            recv_sem=hop_sem.at[step],
            device_id={"seq": lax.rem(me + 2 * step, n)},
            device_id_type=MESH,
        )

    @pl.loop(1, chips)
    def _(step):
        hop(step).start()

    pass_on(me)

    @pl.loop(1, chips)
    def _(step):
        hop(step).wait_recv()
        pass_on(lax.rem(me - 2 * step + n, n))

    await_bytes(fin_ref, chips - 1, send_sem.at[0])
    await_bytes(fin_ref, chips, recv_sem.at[3])
    await_bytes(fin_ref, chips, send_sem.at[3])
    context = rows_together(fin_ref, 0, n).astype(jnp.bfloat16)
    attended = jnp.dot(wout_ref[...], context, preferred_element_type=jnp.float32)
    attended = attended.astype(jnp.bfloat16)
    for step in range(steps):
        out_ref[step] = attended[:, step * per_step : (step + 1) * per_step]


def local(n, frames, dec_states, w_query, w_keyval, w_output, head_slope, lengths, positions):
    steps, frame_count, width = frames.shape
    per_step = dec_states.shape[1]
    tokens = steps * per_step
    heads = head_slope.shape[0]
    size = width // heads
    rows = w_query.shape[1]
    keys = steps * frame_count
    tile = frame_count
    part = math.gcd(width, 256)
    vmem = pl.BlockSpec(memory_space=pltpu.VMEM)
    smem = pl.BlockSpec(memory_space=pltpu.SMEM)
    hbm = pl.BlockSpec(memory_space=pl.ANY)
    out = pl.pallas_call(
        functools.partial(kernel, n),
        out_shape=jax.ShapeDtypeStruct((steps, rows, per_step), jnp.bfloat16),
        in_specs=[vmem, vmem, vmem, vmem, smem, smem, hbm, hbm],
        out_specs=vmem,
        scratch_shapes=[
            pltpu.VMEM((keys // tile, tile, width), jnp.bfloat16),
            pltpu.VMEM((2 * width // part, width, part), jnp.bfloat16),
            pltpu.VMEM((heads, keys, size + EXTRA), jnp.bfloat16),
            pltpu.VMEM((heads, size + EXTRA, keys), jnp.bfloat16),
            pltpu.VMEM((n, rows, tokens), jnp.bfloat16),
            pltpu.VMEM((n, rows, tokens), jnp.bfloat16),
            pltpu.VMEM((n, 4, tokens), jnp.float32),
            pltpu.VMEM((n, rows, tokens), jnp.bfloat16),
            pltpu.VMEM((n, 4, tokens), jnp.float32),
            pltpu.VMEM((n, rows, tokens), jnp.bfloat16),
            pltpu.SemaphoreType.DMA((keys // tile,)),
            pltpu.SemaphoreType.DMA((2 * width // part,)),
            pltpu.SemaphoreType.DMA((4,)),
            pltpu.SemaphoreType.DMA((4,)),
            pltpu.SemaphoreType.DMA((n // 2,)),
        ],
        compiler_params=pltpu.CompilerParams(
            collective_id=0, has_side_effects=True, vmem_limit_bytes=60 * 1024 * 1024
        ),
    )(
        dec_states.reshape(tokens, width),
        w_query.T,
        w_output.T,
        positions.reshape(1, tokens),
        head_slope,
        lengths,
        frames,
        w_keyval,
    )
    return out.transpose(0, 2, 1)


def solution(mesh):
    return jax.shard_map(
        functools.partial(local, mesh.shape["seq"]),
        mesh=mesh,
        in_specs=(
            P("grp", "seq", None),
            P(None, "grp", None),
            P(None, "seq"),
            P(),
            P(None, "seq"),
            P(),
            P("grp", None),
            P(None, "grp"),
        ),
        out_specs=P(None, "grp", "seq"),
        check_vma=False,
    )
```

```python
import functools
import math

import jax
import jax.numpy as jnp
from jax import lax
from jax.experimental import pallas as pl
from jax.experimental.pallas import tpu as pltpu
from jax.sharding import PartitionSpec as P

MESH = pl.DeviceIdType.MESH
EXTRA = 16
MASKED = -1e30


def rows_together(ref, first, count):
    parts = [ref[first + index].astype(jnp.float32) for index in range(count)]
    return jnp.concatenate(parts, axis=0)


def await_bytes(ref, count, sem):
    part = ref.at[pl.ds(0, count)]
    pltpu.make_async_copy(part, part, sem).wait()


def kernel(
    n,
    dec_ref,
    wq_ref,
    wout_ref,
    pos_ref,
    slope_ref,
    len_ref,
    frames_hbm,
    wkv_hbm,
    out_ref,
    frames_ref,
    wkv_ref,
    k_ref,
    vt_ref,
    q_ref,
    ctx_ref,
    stat_ref,
    got_ctx,
    got_stat,
    fin_ref,
    frame_sem,
    weight_sem,
    send_sem,
    recv_sem,
    hop_sem,
):
    me = lax.axis_index("seq")
    steps, frame_count, width = frames_hbm.shape
    tokens = dec_ref.shape[0]
    per_step = tokens // steps
    heads = k_ref.shape[0]
    size = width // heads
    rows = wq_ref.shape[0]
    groups = math.gcd(heads, n)
    group_chunks = n // groups
    group_heads = heads // groups
    tile = frames_ref.shape[1]
    half = wkv_ref.shape[2]
    tiles = frames_ref.shape[0]
    per_block = frame_count // tile
    scale = 1.0 / math.sqrt(size)

    def frame_copy(index):
        return pltpu.make_async_copy(
            frames_hbm.at[index // per_block, pl.ds((index % per_block) * tile, tile)],
            frames_ref.at[index],
            frame_sem.at[index],
        )

    def weight_copy(index):
        return pltpu.make_async_copy(
            wkv_hbm.at[:, pl.ds(pl.multiple_of(index * half, half), half)], wkv_ref.at[index], weight_sem.at[index]
        )

    frame_copy(0).start()
    weight_copy(0).start()
    for index in range(1, tiles):
        frame_copy(index).start()
    for index in range(1, wkv_ref.shape[0]):
        weight_copy(index).start()

    barrier = pltpu.get_barrier_semaphore()

    @pl.loop(1, n)
    def _(step):
        peer = lax.rem(me + step, n)
        pl.semaphore_signal(barrier, inc=1, device_id={"seq": peer}, device_id_type=MESH)

    own_query = lax.dot_general(
        wq_ref[...], dec_ref[...], (((1,), (1,)), ((), ())), preferred_element_type=jnp.float32
    )
    q_ref[me] = own_query.astype(jnp.bfloat16)
    pl.semaphore_wait(barrier, n - 1)

    def send(src, dst, sem, peer):
        pltpu.make_async_remote_copy(
            src_ref=src,
            dst_ref=dst,
            send_sem=send_sem.at[sem],
            recv_sem=recv_sem.at[sem],
            device_id={"seq": peer},
            device_id_type=MESH,
        ).start()

    partner = me + 1 - 2 * lax.rem(me, 2)
    chips = n // 2

    def pass_on(ref, chunk, sem):
        send(ref.at[chunk], ref.at[chunk], sem, partner)

    def hop(ref, step, sem, level):
        return pltpu.make_async_remote_copy(
            src_ref=ref.at[me],
            dst_ref=ref.at[me],
            send_sem=send_sem.at[sem],
            recv_sem=hop_sem.at[level, step],
            device_id={"seq": lax.rem(me + 2 * step, n)},
            device_id_type=MESH,
        )

    def spread(ref, sem, level):
        @pl.loop(1, chips)
        def _(step):
            hop(ref, step, sem, level).start()

        pass_on(ref, me, level)

    def relay(ref, sem, level):
        @pl.loop(1, chips)
        def _(step):
            hop(ref, step, sem, level).wait_recv()
            pass_on(ref, lax.rem(me - 2 * step + n, n), level)

    def settle(ref, sem, level):
        await_bytes(ref, chips - 1, send_sem.at[sem])
        await_bytes(ref, chips, recv_sem.at[level])
        await_bytes(ref, chips, send_sem.at[level])

    spread(q_ref, 2, 0)

    column = lax.broadcasted_iota(jnp.int32, (frame_count, size + EXTRA), 1)
    place = lax.broadcasted_iota(jnp.int32, (frame_count, size + EXTRA), 0)
    masks = []
    for older in range(steps):
        hidden = (place >= len_ref[older, me]) & (column == size)
        masks.append(jnp.where(hidden, MASKED, 0.0).astype(jnp.bfloat16))
    mask = jnp.concatenate(masks, axis=0)
    ones = jnp.ones((EXTRA, steps * frame_count), jnp.bfloat16)

    @pl.loop(0, heads)
    def _(head):
        k_ref[head] = mask
        vt_ref[head, size:, :] = ones

    parts = wkv_ref.shape[0] // 2
    part_heads = half // size

    def project(part, index):
        at = pl.ds(pl.multiple_of(index * tile, tile), tile)
        keyval = jnp.dot(frames_ref[index], wkv_ref[part], preferred_element_type=jnp.float32)
        return at, keyval.astype(jnp.bfloat16)

    for index in range(tiles):
        frame_copy(index).wait()

    @pl.loop(0, parts)
    def _(part):
        weight_copy(part).wait()
        for index in range(tiles):
            at, keyval = project(part, index)
            for local_head in range(part_heads):
                lanes = slice(local_head * size, (local_head + 1) * size)
                k_ref[part * part_heads + local_head, at, 0:size] = keyval[:, lanes]

    def project_values(part):
        weight_copy(parts + part).wait()
        for index in range(tiles):
            at, keyval = project(parts + part, index)
            turned = keyval.T
            for local_head in range(part_heads):
                lanes = slice(local_head * size, (local_head + 1) * size)
                vt_ref[part * part_heads + local_head, 0:size, at] = turned[lanes]

    pl.loop(0, parts - 2)(project_values)
    relay(q_ref, 2, 0)
    pl.loop(parts - 2, parts)(project_values)
    settle(q_ref, 2, 0)

    slot_place = lax.rem(me + 1, n).astype(jnp.float32)
    distance = jnp.abs(pos_ref[...].astype(jnp.float32) - slot_place) / n
    first_row = lax.broadcasted_iota(jnp.int32, (EXTRA, tokens), 0) == 0
    query_tail = jnp.where(first_row, 1.0, 0.0).astype(jnp.bfloat16)
    token_step = lax.broadcasted_iota(jnp.int32, (1, tokens), 1) // per_step

    @pl.loop(0, groups)
    def _(turn):
        group = lax.rem(me // group_chunks + 1 + turn, groups)
        query_rows = rows_together(q_ref, group * group_chunks, group_chunks).astype(jnp.bfloat16)
        peaks, totals, contexts = [], [], []

        def scores(local_head):
            query = jnp.concatenate(
                [query_rows[local_head * size : (local_head + 1) * size], query_tail], axis=0
            )
            return [
                jnp.dot(
                    k_ref[
                        group * group_heads + local_head,
                        pl.ds(older * frame_count, frame_count),
                        :,
                    ],
                    query[:, older * per_step :],
                    preferred_element_type=jnp.float32,
                )
                for older in range(steps)
            ]

        ready = scores(0)
        for local_head in range(group_heads):
            head = group * group_heads + local_head
            raws = ready
            if local_head + 1 < group_heads:
                ready = scores(local_head + 1)
            slope = slope_ref[head]
            peak = context = None
            for older in range(steps):
                first = older * per_step
                block = pl.ds(older * frame_count, frame_count)
                raw = raws[older]
                raw_peak = jnp.max(raw, axis=0, keepdims=True)
                weights = jnp.exp2((raw - raw_peak) * (scale * math.log2(math.e)))
                part_context = jnp.dot(
                    vt_ref[head, :, block],
                    weights.astype(jnp.bfloat16),
                    preferred_element_type=jnp.float32,
                )
                age = (token_step[:, first:] - older).astype(jnp.float32)
                part_peak = raw_peak * scale - slope * (distance[:, first:] + age)
                if peak is None:
                    peak, context = part_peak, part_context
                    continue
                top = jnp.maximum(peak[:, first:], part_peak)
                old_factor = jnp.exp(peak[:, first:] - top)
                new_factor = jnp.exp(part_peak - top)
                merged = context[:, first:] * old_factor + part_context * new_factor
                peak = jnp.concatenate([peak[:, :first], top], axis=1)
                context = jnp.concatenate([context[:, :first], merged], axis=1)
            peaks.append(peak)
            totals.append(context[size : size + 1])
            contexts.append(context[:size])
        stacked = jnp.concatenate(contexts, axis=0)
        for index in range(group_chunks):
            low, high = index * rows, (index + 1) * rows
            one, two = low // size, (high - 1) // size
            chunk = group * group_chunks + index
            ctx_ref[chunk] = stacked[low:high].astype(jnp.bfloat16)
            stat_ref[chunk] = jnp.concatenate(
                [peaks[one], peaks[two], totals[one], totals[two]], axis=0
            )

        @pl.loop(0, group_chunks)
        def _(index):
            chunk = group * group_chunks + lax.rem(me + index, group_chunks)

            @pl.when(chunk != me)
            def _():
                send(stat_ref.at[chunk], got_stat.at[me], 4, chunk)
                send(ctx_ref.at[chunk], got_ctx.at[me], 5, chunk)

    got_stat[me] = stat_ref[me]
    got_ctx[me] = ctx_ref[me]
    await_bytes(got_stat, n - 1, recv_sem.at[4])
    await_bytes(got_ctx, n - 1, recv_sem.at[5])
    await_bytes(stat_ref, n - 1, send_sem.at[4])
    await_bytes(ctx_ref, n - 1, send_sem.at[5])

    top = lax.fori_loop(
        1, n, lambda at, best: jnp.maximum(best, got_stat[at][0:2]), got_stat[0][0:2]
    )
    row = lax.broadcasted_iota(jnp.int32, (rows, tokens), 0)
    is_one = row + lax.rem(me * rows, size) < size

    def add(at, state):
        total, acc = state
        stat = got_stat[at]
        factor = jnp.exp(stat[0:2] - top)
        spread = jnp.where(is_one, factor[0:1], factor[1:2])
        return total + stat[2:4] * factor, acc + got_ctx[at].astype(jnp.float32) * spread

    total, acc = lax.fori_loop(
        0,
        n,
        add,
        (jnp.zeros((2, tokens), jnp.float32), jnp.zeros((rows, tokens), jnp.float32)),
    )
    fin_ref[me] = (acc / jnp.where(is_one, total[0:1], total[1:2])).astype(jnp.bfloat16)

    spread(fin_ref, 3, 1)
    relay(fin_ref, 3, 1)
    settle(fin_ref, 3, 1)
    context = rows_together(fin_ref, 0, n).astype(jnp.bfloat16)
    attended = jnp.dot(wout_ref[...], context, preferred_element_type=jnp.float32)
    attended = attended.astype(jnp.bfloat16)
    for step in range(steps):
        out_ref[step] = attended[:, step * per_step : (step + 1) * per_step]


def local(n, frames, dec_states, w_query, w_keyval, w_output, head_slope, lengths, positions):
    steps, frame_count, width = frames.shape
    per_step = dec_states.shape[1]
    tokens = steps * per_step
    heads = head_slope.shape[0]
    size = width // heads
    rows = w_query.shape[1]
    keys = steps * frame_count
    tile = frame_count
    part = math.gcd(width, 256)
    vmem = pl.BlockSpec(memory_space=pltpu.VMEM)
    smem = pl.BlockSpec(memory_space=pltpu.SMEM)
    hbm = pl.BlockSpec(memory_space=pl.ANY)
    out = pl.pallas_call(
        functools.partial(kernel, n),
        out_shape=jax.ShapeDtypeStruct((steps, rows, per_step), jnp.bfloat16),
        in_specs=[vmem, vmem, vmem, vmem, smem, smem, hbm, hbm],
        out_specs=vmem,
        scratch_shapes=[
            pltpu.VMEM((keys // tile, tile, width), jnp.bfloat16),
            pltpu.VMEM((2 * width // part, width, part), jnp.bfloat16),
            pltpu.VMEM((heads, keys, size + EXTRA), jnp.bfloat16),
            pltpu.VMEM((heads, size + EXTRA, keys), jnp.bfloat16),
            pltpu.VMEM((n, rows, tokens), jnp.bfloat16),
            pltpu.VMEM((n, rows, tokens), jnp.bfloat16),
            pltpu.VMEM((n, 4, tokens), jnp.float32),
            pltpu.VMEM((n, rows, tokens), jnp.bfloat16),
            pltpu.VMEM((n, 4, tokens), jnp.float32),
            pltpu.VMEM((n, rows, tokens), jnp.bfloat16),
            pltpu.SemaphoreType.DMA((keys // tile,)),
            pltpu.SemaphoreType.DMA((2 * width // part,)),
            pltpu.SemaphoreType.DMA((6,)),
            pltpu.SemaphoreType.DMA((6,)),
            pltpu.SemaphoreType.DMA((2, n // 2)),
        ],
        compiler_params=pltpu.CompilerParams(
            collective_id=0, has_side_effects=True, vmem_limit_bytes=60 * 1024 * 1024
        ),
    )(
        dec_states.reshape(tokens, width),
        w_query.T,
        w_output.T,
        positions.reshape(1, tokens),
        head_slope,
        lengths,
        frames,
        w_keyval,
    )
    return out.transpose(0, 2, 1)


def solution(mesh):
    return jax.shard_map(
        functools.partial(local, mesh.shape["seq"]),
        mesh=mesh,
        in_specs=(
            P("grp", "seq", None),
            P(None, "grp", None),
            P(None, "seq"),
            P(),
            P(None, "seq"),
            P(),
            P("grp", None),
            P(None, "grp"),
        ),
        out_specs=P(None, "grp", "seq"),
        check_vma=False,
    )
```

```python
import functools
import math

import jax
import jax.numpy as jnp
from jax import lax
from jax.experimental import pallas as pl
from jax.experimental.pallas import tpu as pltpu
from jax.sharding import PartitionSpec as P

MESH = pl.DeviceIdType.MESH
EXTRA = 16
MASKED = -1e30


def rows_together(ref, first, count):
    parts = [ref[first + index].astype(jnp.float32) for index in range(count)]
    return jnp.concatenate(parts, axis=0)


def await_bytes(ref, count, sem):
    part = ref.at[pl.ds(0, count)]
    pltpu.make_async_copy(part, part, sem).wait()


def kernel(
    n,
    dec_ref,
    wq_ref,
    wout_ref,
    pos_ref,
    slope_ref,
    len_ref,
    frames_hbm,
    wkv_hbm,
    out_ref,
    frames_ref,
    wkv_ref,
    k_ref,
    vt_ref,
    q_ref,
    ctx_ref,
    stat_ref,
    got_ctx,
    got_stat,
    pair_ctx,
    pair_stat,
    sum_ctx,
    sum_stat,
    fin_ref,
    frame_sem,
    weight_sem,
    send_sem,
    recv_sem,
    hop_sem,
    pair_sem,
):
    me = lax.axis_index("seq")
    steps, frame_count, width = frames_hbm.shape
    tokens = dec_ref.shape[0]
    per_step = tokens // steps
    heads = k_ref.shape[0]
    size = width // heads
    rows = wq_ref.shape[0]
    groups = math.gcd(heads, n)
    group_chunks = n // groups
    group_heads = heads // groups
    tile = frames_ref.shape[1]
    half = wkv_ref.shape[2]
    tiles = frames_ref.shape[0]
    per_block = frame_count // tile
    scale = 1.0 / math.sqrt(size)

    def frame_copy(index):
        return pltpu.make_async_copy(
            frames_hbm.at[index // per_block, pl.ds((index % per_block) * tile, tile)],
            frames_ref.at[index],
            frame_sem.at[index],
        )

    def weight_copy(index):
        return pltpu.make_async_copy(
            wkv_hbm.at[:, pl.ds(pl.multiple_of(index * half, half), half)], wkv_ref.at[index], weight_sem.at[index]
        )

    frame_copy(0).start()
    weight_copy(0).start()
    for index in range(1, tiles):
        frame_copy(index).start()
    for index in range(1, wkv_ref.shape[0]):
        weight_copy(index).start()

    barrier = pltpu.get_barrier_semaphore()

    @pl.loop(1, n)
    def _(step):
        peer = lax.rem(me + step, n)
        pl.semaphore_signal(barrier, inc=1, device_id={"seq": peer}, device_id_type=MESH)

    own_query = lax.dot_general(
        wq_ref[...], dec_ref[...], (((1,), (1,)), ((), ())), preferred_element_type=jnp.float32
    )
    q_ref[me] = own_query.astype(jnp.bfloat16)
    pl.semaphore_wait(barrier, n - 1)

    def send(src, dst, sem, peer):
        pltpu.make_async_remote_copy(
            src_ref=src,
            dst_ref=dst,
            send_sem=send_sem.at[sem],
            recv_sem=recv_sem.at[sem],
            device_id={"seq": peer},
            device_id_type=MESH,
        ).start()

    partner = me + 1 - 2 * lax.rem(me, 2)
    chips = n // 2

    def pass_on(ref, chunk, sem):
        send(ref.at[chunk], ref.at[chunk], sem, partner)

    def hop(ref, step, sem, level):
        return pltpu.make_async_remote_copy(
            src_ref=ref.at[me],
            dst_ref=ref.at[me],
            send_sem=send_sem.at[sem],
            recv_sem=hop_sem.at[level, step],
            device_id={"seq": lax.rem(me + 2 * step, n)},
            device_id_type=MESH,
        )

    def spread(ref, sem, level):
        @pl.loop(1, chips)
        def _(step):
            hop(ref, step, sem, level).start()

        pass_on(ref, me, level)

    def relay(ref, sem, level):
        @pl.loop(1, chips)
        def _(step):
            hop(ref, step, sem, level).wait_recv()
            pass_on(ref, lax.rem(me - 2 * step + n, n), level)

    def settle(ref, sem, level):
        await_bytes(ref, chips - 1, send_sem.at[sem])
        await_bytes(ref, chips, recv_sem.at[level])
        await_bytes(ref, chips, send_sem.at[level])

    spread(q_ref, 2, 0)

    column = lax.broadcasted_iota(jnp.int32, (frame_count, size + EXTRA), 1)
    place = lax.broadcasted_iota(jnp.int32, (frame_count, size + EXTRA), 0)
    masks = []
    for older in range(steps):
        hidden = (place >= len_ref[older, me]) & (column == size)
        masks.append(jnp.where(hidden, MASKED, 0.0).astype(jnp.bfloat16))
    mask = jnp.concatenate(masks, axis=0)
    ones = jnp.ones((EXTRA, steps * frame_count), jnp.bfloat16)

    @pl.loop(0, heads)
    def _(head):
        k_ref[head] = mask
        vt_ref[head, size:, :] = ones

    parts = wkv_ref.shape[0] // 2
    part_heads = half // size

    def project(part, index):
        at = pl.ds(pl.multiple_of(index * tile, tile), tile)
        keyval = jnp.dot(frames_ref[index], wkv_ref[part], preferred_element_type=jnp.float32)
        return at, keyval.astype(jnp.bfloat16)

    for index in range(tiles):
        frame_copy(index).wait()

    @pl.loop(0, parts)
    def _(part):
        weight_copy(part).wait()
        for index in range(tiles):
            at, keyval = project(part, index)
            for local_head in range(part_heads):
                lanes = slice(local_head * size, (local_head + 1) * size)
                k_ref[part * part_heads + local_head, at, 0:size] = keyval[:, lanes]

    def project_values(part):
        weight_copy(parts + part).wait()
        for index in range(tiles):
            at, keyval = project(parts + part, index)
            turned = keyval.T
            for local_head in range(part_heads):
                lanes = slice(local_head * size, (local_head + 1) * size)
                vt_ref[part * part_heads + local_head, 0:size, at] = turned[lanes]

    pl.loop(0, parts - 2)(project_values)
    relay(q_ref, 2, 0)
    pl.loop(parts - 2, parts)(project_values)
    settle(q_ref, 2, 0)

    slot_place = lax.rem(me + 1, n).astype(jnp.float32)
    distance = jnp.abs(pos_ref[...].astype(jnp.float32) - slot_place) / n
    first_row = lax.broadcasted_iota(jnp.int32, (EXTRA, tokens), 0) == 0
    query_tail = jnp.where(first_row, 1.0, 0.0).astype(jnp.bfloat16)
    token_step = lax.broadcasted_iota(jnp.int32, (1, tokens), 1) // per_step

    row = lax.broadcasted_iota(jnp.int32, (rows, tokens), 0)

    def pass_sums(turn):
        group = lax.rem(me // group_chunks + 1 + turn, groups)
        await_bytes(pair_stat, group_chunks // 2, pair_sem.at[0, turn])
        await_bytes(pair_ctx, group_chunks // 2, pair_sem.at[1, turn])

        @pl.loop(0, group_chunks // 2)
        def _(index):
            chunk = group * group_chunks + 2 * index + lax.rem(me, 2)
            slot = chunk // 2
            one, two = stat_ref[chunk], pair_stat[slot]
            top = jnp.maximum(one[0:2], two[0:2])
            one_factor = jnp.exp(one[0:2] - top)
            two_factor = jnp.exp(two[0:2] - top)
            stat = jnp.concatenate([top, one[2:4] * one_factor + two[2:4] * two_factor], axis=0)
            is_one = row + lax.rem(chunk * rows, size) < size
            context = ctx_ref[chunk].astype(jnp.float32) * jnp.where(
                is_one, one_factor[0:1], one_factor[1:2]
            ) + pair_ctx[slot].astype(jnp.float32) * jnp.where(
                is_one, two_factor[0:1], two_factor[1:2]
            )
            context = context.astype(jnp.bfloat16)

            @pl.when(chunk != me)
            def _():
                sum_stat[slot] = stat
                sum_ctx[slot] = context
                send(sum_stat.at[slot], got_stat.at[me // 2], 4, chunk)
                send(sum_ctx.at[slot], got_ctx.at[me // 2], 5, chunk)

            @pl.when(chunk == me)
            def _():
                got_stat[slot] = stat
                got_ctx[slot] = context

    @pl.loop(0, groups)
    def _(turn):
        group = lax.rem(me // group_chunks + 1 + turn, groups)
        query_rows = rows_together(q_ref, group * group_chunks, group_chunks).astype(jnp.bfloat16)
        peaks, totals, contexts = [], [], []

        def scores(local_head):
            query = jnp.concatenate(
                [query_rows[local_head * size : (local_head + 1) * size], query_tail], axis=0
            )
            return [
                jnp.dot(
                    k_ref[
                        group * group_heads + local_head,
                        pl.ds(older * frame_count, frame_count),
                        :,
                    ],
                    query[:, older * per_step :],
                    preferred_element_type=jnp.float32,
                )
                for older in range(steps)
            ]

        ready = scores(0)
        for local_head in range(group_heads):
            head = group * group_heads + local_head
            raws = ready
            if local_head + 1 < group_heads:
                ready = scores(local_head + 1)
            slope = slope_ref[head]
            peak = context = None
            for older in range(steps):
                first = older * per_step
                block = pl.ds(older * frame_count, frame_count)
                raw = raws[older]
                raw_peak = jnp.max(raw, axis=0, keepdims=True)
                weights = jnp.exp2((raw - raw_peak) * (scale * math.log2(math.e)))
                part_context = jnp.dot(
                    vt_ref[head, :, block],
                    weights.astype(jnp.bfloat16),
                    preferred_element_type=jnp.float32,
                )
                age = (token_step[:, first:] - older).astype(jnp.float32)
                part_peak = raw_peak * scale - slope * (distance[:, first:] + age)
                if peak is None:
                    peak, context = part_peak, part_context
                    continue
                top = jnp.maximum(peak[:, first:], part_peak)
                old_factor = jnp.exp(peak[:, first:] - top)
                new_factor = jnp.exp(part_peak - top)
                merged = context[:, first:] * old_factor + part_context * new_factor
                peak = jnp.concatenate([peak[:, :first], top], axis=1)
                context = jnp.concatenate([context[:, :first], merged], axis=1)
            peaks.append(peak)
            totals.append(context[size : size + 1])
            contexts.append(context[:size])
        stacked = jnp.concatenate(contexts, axis=0)
        for index in range(group_chunks):
            low, high = index * rows, (index + 1) * rows
            one, two = low // size, (high - 1) // size
            chunk = group * group_chunks + index
            ctx_ref[chunk] = stacked[low:high].astype(jnp.bfloat16)
            stat_ref[chunk] = jnp.concatenate(
                [peaks[one], peaks[two], totals[one], totals[two]], axis=0
            )

        @pl.loop(0, group_chunks // 2)
        def _(index):
            chunk = group * group_chunks + 2 * index + 1 - lax.rem(me, 2)
            for kind, (src, dst) in enumerate(((stat_ref, pair_stat), (ctx_ref, pair_ctx))):
                pltpu.make_async_remote_copy(
                    src_ref=src.at[chunk],
                    dst_ref=dst.at[chunk // 2],
                    send_sem=send_sem.at[kind],
                    recv_sem=pair_sem.at[kind, turn],
                    device_id={"seq": partner},
                    device_id_type=MESH,
                ).start()

        @pl.when(turn > 0)
        def _():
            pass_sums(turn - 1)

    pass_sums(groups - 1)
    await_bytes(got_stat, chips - 1, recv_sem.at[4])
    await_bytes(got_ctx, chips - 1, recv_sem.at[5])
    await_bytes(sum_stat, chips - 1, send_sem.at[4])
    await_bytes(sum_ctx, chips - 1, send_sem.at[5])
    await_bytes(stat_ref, chips, send_sem.at[0])
    await_bytes(ctx_ref, chips, send_sem.at[1])

    top = lax.fori_loop(
        1, chips, lambda at, best: jnp.maximum(best, got_stat[at][0:2]), got_stat[0][0:2]
    )
    is_one = row + lax.rem(me * rows, size) < size

    def add(at, state):
        total, acc = state
        stat = got_stat[at]
        factor = jnp.exp(stat[0:2] - top)
        spread = jnp.where(is_one, factor[0:1], factor[1:2])
        return total + stat[2:4] * factor, acc + got_ctx[at].astype(jnp.float32) * spread

    total, acc = lax.fori_loop(
        0,
        chips,
        add,
        (jnp.zeros((2, tokens), jnp.float32), jnp.zeros((rows, tokens), jnp.float32)),
    )
    fin_ref[me] = (acc / jnp.where(is_one, total[0:1], total[1:2])).astype(jnp.bfloat16)

    spread(fin_ref, 3, 1)
    relay(fin_ref, 3, 1)
    settle(fin_ref, 3, 1)
    context = rows_together(fin_ref, 0, n).astype(jnp.bfloat16)
    attended = jnp.dot(wout_ref[...], context, preferred_element_type=jnp.float32)
    attended = attended.astype(jnp.bfloat16)
    for step in range(steps):
        out_ref[step] = attended[:, step * per_step : (step + 1) * per_step]


def local(n, frames, dec_states, w_query, w_keyval, w_output, head_slope, lengths, positions):
    steps, frame_count, width = frames.shape
    per_step = dec_states.shape[1]
    tokens = steps * per_step
    heads = head_slope.shape[0]
    size = width // heads
    rows = w_query.shape[1]
    keys = steps * frame_count
    tile = frame_count
    part = math.gcd(width, 256)
    vmem = pl.BlockSpec(memory_space=pltpu.VMEM)
    smem = pl.BlockSpec(memory_space=pltpu.SMEM)
    hbm = pl.BlockSpec(memory_space=pl.ANY)
    out = pl.pallas_call(
        functools.partial(kernel, n),
        out_shape=jax.ShapeDtypeStruct((steps, rows, per_step), jnp.bfloat16),
        in_specs=[vmem, vmem, vmem, vmem, smem, smem, hbm, hbm],
        out_specs=vmem,
        scratch_shapes=[
            pltpu.VMEM((keys // tile, tile, width), jnp.bfloat16),
            pltpu.VMEM((2 * width // part, width, part), jnp.bfloat16),
            pltpu.VMEM((heads, keys, size + EXTRA), jnp.bfloat16),
            pltpu.VMEM((heads, size + EXTRA, keys), jnp.bfloat16),
            pltpu.VMEM((n, rows, tokens), jnp.bfloat16),
            pltpu.VMEM((n, rows, tokens), jnp.bfloat16),
            pltpu.VMEM((n, 4, tokens), jnp.float32),
            pltpu.VMEM((n // 2, rows, tokens), jnp.bfloat16),
            pltpu.VMEM((n // 2, 4, tokens), jnp.float32),
            pltpu.VMEM((n // 2, rows, tokens), jnp.bfloat16),
            pltpu.VMEM((n // 2, 4, tokens), jnp.float32),
            pltpu.VMEM((n // 2, rows, tokens), jnp.bfloat16),
            pltpu.VMEM((n // 2, 4, tokens), jnp.float32),
            pltpu.VMEM((n, rows, tokens), jnp.bfloat16),
            pltpu.SemaphoreType.DMA((keys // tile,)),
            pltpu.SemaphoreType.DMA((2 * width // part,)),
            pltpu.SemaphoreType.DMA((6,)),
            pltpu.SemaphoreType.DMA((6,)),
            pltpu.SemaphoreType.DMA((2, n // 2)),
            pltpu.SemaphoreType.DMA((2, math.gcd(heads, n))),
        ],
        compiler_params=pltpu.CompilerParams(
            collective_id=0, has_side_effects=True, vmem_limit_bytes=60 * 1024 * 1024
        ),
    )(
        dec_states.reshape(tokens, width),
        w_query.T,
        w_output.T,
        positions.reshape(1, tokens),
        head_slope,
        lengths,
        frames,
        w_keyval,
    )
    return out.transpose(0, 2, 1)


def solution(mesh):
    return jax.shard_map(
        functools.partial(local, mesh.shape["seq"]),
        mesh=mesh,
        in_specs=(
            P("grp", "seq", None),
            P(None, "grp", None),
            P(None, "seq"),
            P(),
            P(None, "seq"),
            P(),
            P("grp", None),
            P(None, "grp"),
        ),
        out_specs=P(None, "grp", "seq"),
        check_vma=False,
    )
```

```python
import functools
import math

import jax
import jax.numpy as jnp
from jax import lax
from jax.experimental import pallas as pl
from jax.experimental.pallas import tpu as pltpu
from jax.sharding import PartitionSpec as P

MESH = pl.DeviceIdType.MESH
EXTRA = 16
MASKED = -1e30


def rows_together(ref, first, count):
    parts = [ref[first + index].astype(jnp.float32) for index in range(count)]
    return jnp.concatenate(parts, axis=0)


def await_bytes(ref, count, sem):
    part = ref.at[pl.ds(0, count)]
    pltpu.make_async_copy(part, part, sem).wait()


def kernel(
    n,
    dec_ref,
    wq_ref,
    wout_ref,
    pos_ref,
    slope_ref,
    len_ref,
    frames_hbm,
    wkv_hbm,
    out_ref,
    frames_ref,
    wkv_ref,
    k_ref,
    vt_ref,
    q_ref,
    ctx_ref,
    stat_ref,
    got_ctx,
    got_stat,
    pair_ctx,
    pair_stat,
    sum_ctx,
    sum_stat,
    fin_ref,
    frame_sem,
    weight_sem,
    send_sem,
    recv_sem,
    hop_sem,
    pair_sem,
):
    me = lax.axis_index("seq")
    steps, frame_count, width = frames_hbm.shape
    tokens = dec_ref.shape[0]
    per_step = tokens // steps
    heads = k_ref.shape[0]
    size = width // heads
    rows = wq_ref.shape[0]
    groups = math.gcd(heads, n)
    group_chunks = n // groups
    group_heads = heads // groups
    tile = frames_ref.shape[1]
    half = wkv_ref.shape[2]
    tiles = frames_ref.shape[0]
    per_block = frame_count // tile
    scale = 1.0 / math.sqrt(size)

    def frame_copy(index):
        return pltpu.make_async_copy(
            frames_hbm.at[index // per_block, pl.ds((index % per_block) * tile, tile)],
            frames_ref.at[index],
            frame_sem.at[index],
        )

    def weight_copy(index):
        return pltpu.make_async_copy(
            wkv_hbm.at[:, pl.ds(pl.multiple_of(index * half, half), half)], wkv_ref.at[index], weight_sem.at[index]
        )

    barrier = pltpu.get_barrier_semaphore()

    @pl.loop(1, n)
    def _(step):
        peer = lax.rem(me + step, n)
        pl.semaphore_signal(barrier, inc=1, device_id={"seq": peer}, device_id_type=MESH)

    frame_copy(0).start()
    weight_copy(0).start()
    for index in range(1, tiles):
        frame_copy(index).start()
    for index in range(1, wkv_ref.shape[0]):
        weight_copy(index).start()

    own_query = lax.dot_general(
        wq_ref[...], dec_ref[...], (((1,), (1,)), ((), ())), preferred_element_type=jnp.float32
    )
    q_ref[me] = own_query.astype(jnp.bfloat16)
    pl.semaphore_wait(barrier, n - 1)

    def send(src, dst, sem, peer):
        pltpu.make_async_remote_copy(
            src_ref=src,
            dst_ref=dst,
            send_sem=send_sem.at[sem],
            recv_sem=recv_sem.at[sem],
            device_id={"seq": peer},
            device_id_type=MESH,
        ).start()

    partner = me + 1 - 2 * lax.rem(me, 2)
    chips = n // 2

    def pass_on(ref, chunk, sem):
        send(ref.at[chunk], ref.at[chunk], sem, partner)

    columns = n // 4
    beside = me + 2 - 4 * lax.rem(me // 2, 2)

    def hop(ref, step, sem, level):
        return pltpu.make_async_remote_copy(
            src_ref=ref.at[me],
            dst_ref=ref.at[me],
            send_sem=send_sem.at[sem],
            recv_sem=hop_sem.at[level, step],
            device_id={"seq": lax.rem(me + 4 * step, n)},
            device_id_type=MESH,
        )

    def cross(ref, step, sem, level):
        chunk = lax.rem(me - 4 * step + n, n)
        return pltpu.make_async_remote_copy(
            src_ref=ref.at[chunk],
            dst_ref=ref.at[chunk],
            send_sem=send_sem.at[sem],
            recv_sem=hop_sem.at[level, columns + step],
            device_id={"seq": beside},
            device_id_type=MESH,
        )

    def spread(ref, sem, level):
        @pl.loop(1, columns)
        def _(step):
            hop(ref, step, sem, level).start()

        cross(ref, 0, sem, level).start()
        pass_on(ref, me, level)

    def relay(ref, sem, level):
        @pl.loop(1, columns)
        def _(step):
            hop(ref, step, sem, level).wait_recv()
            cross(ref, step, sem, level).start()
            pass_on(ref, lax.rem(me - 4 * step + n, n), level)

        @pl.loop(0, columns)
        def _(step):
            cross(ref, step, sem, level).wait_recv()
            pass_on(ref, lax.rem(beside - 4 * step + n, n), level)

    def settle(ref, sem, level):
        await_bytes(ref, chips - 1, send_sem.at[sem])
        await_bytes(ref, chips, recv_sem.at[level])
        await_bytes(ref, chips, send_sem.at[level])

    spread(q_ref, 2, 0)

    column = lax.broadcasted_iota(jnp.int32, (frame_count, size + EXTRA), 1)
    place = lax.broadcasted_iota(jnp.int32, (frame_count, size + EXTRA), 0)
    masks = []
    for older in range(steps):
        hidden = (place >= len_ref[older, me]) & (column == size)
        masks.append(jnp.where(hidden, MASKED, 0.0).astype(jnp.bfloat16))
    mask = jnp.concatenate(masks, axis=0)
    ones = jnp.ones((EXTRA, steps * frame_count), jnp.bfloat16)

    @pl.loop(0, heads)
    def _(head):
        k_ref[head] = mask
        vt_ref[head, size:, :] = ones

    parts = wkv_ref.shape[0] // 2
    part_heads = half // size

    def project(part, index):
        at = pl.ds(pl.multiple_of(index * tile, tile), tile)
        keyval = jnp.dot(frames_ref[index], wkv_ref[part], preferred_element_type=jnp.float32)
        return at, keyval.astype(jnp.bfloat16)

    for index in range(tiles):
        frame_copy(index).wait()

    @pl.loop(0, parts)
    def _(part):
        weight_copy(part).wait()
        for index in range(tiles):
            at, keyval = project(part, index)
            for local_head in range(part_heads):
                lanes = slice(local_head * size, (local_head + 1) * size)
                k_ref[part * part_heads + local_head, at, 0:size] = keyval[:, lanes]

    def project_values(part):
        weight_copy(parts + part).wait()
        for index in range(tiles):
            at, keyval = project(parts + part, index)
            turned = keyval.T
            for local_head in range(part_heads):
                lanes = slice(local_head * size, (local_head + 1) * size)
                vt_ref[part * part_heads + local_head, 0:size, at] = turned[lanes]

    pl.loop(0, parts - 2)(project_values)
    relay(q_ref, 2, 0)
    pl.loop(parts - 2, parts)(project_values)
    settle(q_ref, 2, 0)

    slot_place = lax.rem(me + 1, n).astype(jnp.float32)
    distance = jnp.abs(pos_ref[...].astype(jnp.float32) - slot_place) / n
    first_row = lax.broadcasted_iota(jnp.int32, (EXTRA, tokens), 0) == 0
    query_tail = jnp.where(first_row, 1.0, 0.0).astype(jnp.bfloat16)
    token_step = lax.broadcasted_iota(jnp.int32, (1, tokens), 1) // per_step

    row = lax.broadcasted_iota(jnp.int32, (rows, tokens), 0)

    def pass_sums(turn):
        group = lax.rem(me // group_chunks + 1 + turn, groups)
        await_bytes(pair_stat, group_chunks // 2, pair_sem.at[0, turn])
        await_bytes(pair_ctx, group_chunks // 2, pair_sem.at[1, turn])

        @pl.loop(0, group_chunks // 2)
        def _(index):
            chunk = group * group_chunks + 2 * index + lax.rem(me, 2)
            slot = chunk // 2
            one, two = stat_ref[chunk], pair_stat[slot]
            top = jnp.maximum(one[0:2], two[0:2])
            one_factor = jnp.exp(one[0:2] - top)
            two_factor = jnp.exp(two[0:2] - top)
            stat = jnp.concatenate([top, one[2:4] * one_factor + two[2:4] * two_factor], axis=0)
            is_one = row + lax.rem(chunk * rows, size) < size
            context = ctx_ref[chunk].astype(jnp.float32) * jnp.where(
                is_one, one_factor[0:1], one_factor[1:2]
            ) + pair_ctx[slot].astype(jnp.float32) * jnp.where(
                is_one, two_factor[0:1], two_factor[1:2]
            )
            context = context.astype(jnp.bfloat16)

            @pl.when(chunk != me)
            def _():
                sum_stat[slot] = stat
                sum_ctx[slot] = context
                send(sum_stat.at[slot], got_stat.at[me // 2], 4, chunk)
                send(sum_ctx.at[slot], got_ctx.at[me // 2], 5, chunk)

            @pl.when(chunk == me)
            def _():
                got_stat[slot] = stat
                got_ctx[slot] = context

    @pl.loop(0, groups)
    def _(turn):
        group = lax.rem(me // group_chunks + 1 + turn, groups)
        query_rows = rows_together(q_ref, group * group_chunks, group_chunks).astype(jnp.bfloat16)
        peaks, totals, contexts = [], [], []

        def scores(local_head):
            query = jnp.concatenate(
                [query_rows[local_head * size : (local_head + 1) * size], query_tail], axis=0
            )
            return [
                jnp.dot(
                    k_ref[
                        group * group_heads + local_head,
                        pl.ds(older * frame_count, frame_count),
                        :,
                    ],
                    query[:, older * per_step :],
                    preferred_element_type=jnp.float32,
                )
                for older in range(steps)
            ]

        ready = scores(0)
        for local_head in range(group_heads):
            head = group * group_heads + local_head
            raws = ready
            if local_head + 1 < group_heads:
                ready = scores(local_head + 1)
            slope = slope_ref[head]
            peak = context = None
            for older in range(steps):
                first = older * per_step
                block = pl.ds(older * frame_count, frame_count)
                raw = raws[older]
                raw_peak = jnp.max(raw, axis=0, keepdims=True)
                weights = jnp.exp2((raw - raw_peak) * (scale * math.log2(math.e)))
                part_context = jnp.dot(
                    vt_ref[head, :, block],
                    weights.astype(jnp.bfloat16),
                    preferred_element_type=jnp.float32,
                )
                age = (token_step[:, first:] - older).astype(jnp.float32)
                part_peak = raw_peak * scale - slope * (distance[:, first:] + age)
                if peak is None:
                    peak, context = part_peak, part_context
                    continue
                top = jnp.maximum(peak[:, first:], part_peak)
                old_factor = jnp.exp(peak[:, first:] - top)
                new_factor = jnp.exp(part_peak - top)
                merged = context[:, first:] * old_factor + part_context * new_factor
                peak = jnp.concatenate([peak[:, :first], top], axis=1)
                context = jnp.concatenate([context[:, :first], merged], axis=1)
            peaks.append(peak)
            totals.append(context[size : size + 1])
            contexts.append(context[:size])
        stacked = jnp.concatenate(contexts, axis=0)
        for index in range(group_chunks):
            low, high = index * rows, (index + 1) * rows
            one, two = low // size, (high - 1) // size
            chunk = group * group_chunks + index
            ctx_ref[chunk] = stacked[low:high].astype(jnp.bfloat16)
            stat_ref[chunk] = jnp.concatenate(
                [peaks[one], peaks[two], totals[one], totals[two]], axis=0
            )

        @pl.loop(0, group_chunks // 2)
        def _(index):
            chunk = group * group_chunks + 2 * index + 1 - lax.rem(me, 2)
            for kind, (src, dst) in enumerate(((stat_ref, pair_stat), (ctx_ref, pair_ctx))):
                pltpu.make_async_remote_copy(
                    src_ref=src.at[chunk],
                    dst_ref=dst.at[chunk // 2],
                    send_sem=send_sem.at[kind],
                    recv_sem=pair_sem.at[kind, turn],
                    device_id={"seq": partner},
                    device_id_type=MESH,
                ).start()

        @pl.when(turn > 0)
        def _():
            pass_sums(turn - 1)

    pass_sums(groups - 1)
    await_bytes(got_stat, chips - 1, recv_sem.at[4])
    await_bytes(got_ctx, chips - 1, recv_sem.at[5])
    await_bytes(sum_stat, chips - 1, send_sem.at[4])
    await_bytes(sum_ctx, chips - 1, send_sem.at[5])
    await_bytes(stat_ref, chips, send_sem.at[0])
    await_bytes(ctx_ref, chips, send_sem.at[1])

    top = lax.fori_loop(
        1, chips, lambda at, best: jnp.maximum(best, got_stat[at][0:2]), got_stat[0][0:2]
    )
    is_one = row + lax.rem(me * rows, size) < size

    def add(at, state):
        total, acc = state
        stat = got_stat[at]
        factor = jnp.exp(stat[0:2] - top)
        spread = jnp.where(is_one, factor[0:1], factor[1:2])
        return total + stat[2:4] * factor, acc + got_ctx[at].astype(jnp.float32) * spread

    total, acc = lax.fori_loop(
        0,
        chips,
        add,
        (jnp.zeros((2, tokens), jnp.float32), jnp.zeros((rows, tokens), jnp.float32)),
    )
    fin_ref[me] = (acc / jnp.where(is_one, total[0:1], total[1:2])).astype(jnp.bfloat16)

    spread(fin_ref, 3, 1)
    relay(fin_ref, 3, 1)
    settle(fin_ref, 3, 1)
    context = rows_together(fin_ref, 0, n).astype(jnp.bfloat16)
    attended = jnp.dot(wout_ref[...], context, preferred_element_type=jnp.float32)
    attended = attended.astype(jnp.bfloat16)
    for step in range(steps):
        out_ref[step] = attended[:, step * per_step : (step + 1) * per_step]


def local(n, frames, dec_states, w_query, w_keyval, w_output, head_slope, lengths, positions):
    steps, frame_count, width = frames.shape
    per_step = dec_states.shape[1]
    tokens = steps * per_step
    heads = head_slope.shape[0]
    size = width // heads
    rows = w_query.shape[1]
    keys = steps * frame_count
    tile = frame_count
    part = math.gcd(width, 256)
    vmem = pl.BlockSpec(memory_space=pltpu.VMEM)
    smem = pl.BlockSpec(memory_space=pltpu.SMEM)
    hbm = pl.BlockSpec(memory_space=pl.ANY)
    out = pl.pallas_call(
        functools.partial(kernel, n),
        out_shape=jax.ShapeDtypeStruct((steps, rows, per_step), jnp.bfloat16),
        in_specs=[vmem, vmem, vmem, vmem, smem, smem, hbm, hbm],
        out_specs=vmem,
        scratch_shapes=[
            pltpu.VMEM((keys // tile, tile, width), jnp.bfloat16),
            pltpu.VMEM((2 * width // part, width, part), jnp.bfloat16),
            pltpu.VMEM((heads, keys, size + EXTRA), jnp.bfloat16),
            pltpu.VMEM((heads, size + EXTRA, keys), jnp.bfloat16),
            pltpu.VMEM((n, rows, tokens), jnp.bfloat16),
            pltpu.VMEM((n, rows, tokens), jnp.bfloat16),
            pltpu.VMEM((n, 4, tokens), jnp.float32),
            pltpu.VMEM((n // 2, rows, tokens), jnp.bfloat16),
            pltpu.VMEM((n // 2, 4, tokens), jnp.float32),
            pltpu.VMEM((n // 2, rows, tokens), jnp.bfloat16),
            pltpu.VMEM((n // 2, 4, tokens), jnp.float32),
            pltpu.VMEM((n // 2, rows, tokens), jnp.bfloat16),
            pltpu.VMEM((n // 2, 4, tokens), jnp.float32),
            pltpu.VMEM((n, rows, tokens), jnp.bfloat16),
            pltpu.SemaphoreType.DMA((keys // tile,)),
            pltpu.SemaphoreType.DMA((2 * width // part,)),
            pltpu.SemaphoreType.DMA((6,)),
            pltpu.SemaphoreType.DMA((6,)),
            pltpu.SemaphoreType.DMA((2, n // 2)),
            pltpu.SemaphoreType.DMA((2, math.gcd(heads, n))),
        ],
        compiler_params=pltpu.CompilerParams(
            collective_id=0, has_side_effects=True, vmem_limit_bytes=60 * 1024 * 1024
        ),
    )(
        dec_states.reshape(tokens, width),
        w_query.T,
        w_output.T,
        positions.reshape(1, tokens),
        head_slope,
        lengths,
        frames,
        w_keyval,
    )
    return out.transpose(0, 2, 1)


def solution(mesh):
    return jax.shard_map(
        functools.partial(local, mesh.shape["seq"]),
        mesh=mesh,
        in_specs=(
            P("grp", "seq", None),
            P(None, "grp", None),
            P(None, "seq"),
            P(),
            P(None, "seq"),
            P(),
            P("grp", None),
            P(None, "grp"),
        ),
        out_specs=P(None, "grp", "seq"),
        check_vma=False,
    )
```

```python
import functools
import math

import jax
import jax.numpy as jnp
from jax import lax
from jax.experimental import pallas as pl
from jax.experimental.pallas import tpu as pltpu
from jax.sharding import PartitionSpec as P

MESH = pl.DeviceIdType.MESH
EXTRA = 16
MASKED = -1e30


def rows_together(ref, first, count):
    parts = [ref[first + index].astype(jnp.float32) for index in range(count)]
    return jnp.concatenate(parts, axis=0)


def await_bytes(ref, count, sem):
    part = ref.at[pl.ds(0, count)]
    pltpu.make_async_copy(part, part, sem).wait()


def kernel(
    n,
    dec_ref,
    wq_ref,
    wout_ref,
    pos_ref,
    slope_ref,
    len_ref,
    frames_hbm,
    wkv_hbm,
    out_ref,
    frames_ref,
    wkv_ref,
    k_ref,
    vt_ref,
    q_ref,
    ctx_ref,
    stat_ref,
    got_ctx,
    got_stat,
    pair_ctx,
    pair_stat,
    sum_ctx,
    sum_stat,
    fin_ref,
    frame_sem,
    weight_sem,
    send_sem,
    recv_sem,
    hop_sem,
    pair_sem,
):
    me = lax.axis_index("seq")
    steps, frame_count, width = frames_hbm.shape
    tokens = dec_ref.shape[0]
    per_step = tokens // steps
    heads = k_ref.shape[0]
    size = width // heads
    rows = wq_ref.shape[0]
    groups = math.gcd(heads, n)
    group_chunks = n // groups
    group_heads = heads // groups
    tile = frames_ref.shape[1]
    half = wkv_ref.shape[2]
    tiles = frames_ref.shape[0]
    per_block = frame_count // tile
    scale = 1.0 / math.sqrt(size)

    def frame_copy(index):
        return pltpu.make_async_copy(
            frames_hbm.at[index // per_block, pl.ds((index % per_block) * tile, tile)],
            frames_ref.at[index],
            frame_sem.at[index],
        )

    def weight_copy(index):
        return pltpu.make_async_copy(
            wkv_hbm.at[:, pl.ds(pl.multiple_of(index * half, half), half)], wkv_ref.at[index], weight_sem.at[index]
        )

    frame_copy(0).start()
    weight_copy(0).start()
    for index in range(1, tiles):
        frame_copy(index).start()
    for index in range(1, wkv_ref.shape[0]):
        weight_copy(index).start()

    barrier = pltpu.get_barrier_semaphore()

    @pl.loop(1, n)
    def _(step):
        peer = lax.rem(me + step, n)
        pl.semaphore_signal(barrier, inc=1, device_id={"seq": peer}, device_id_type=MESH)

    own_query = lax.dot_general(
        wq_ref[...], dec_ref[...], (((1,), (1,)), ((), ())), preferred_element_type=jnp.float32
    )
    q_ref[me] = own_query.astype(jnp.bfloat16)
    pl.semaphore_wait(barrier, n - 1)

    def send(src, dst, sem, peer):
        pltpu.make_async_remote_copy(
            src_ref=src,
            dst_ref=dst,
            send_sem=send_sem.at[sem],
            recv_sem=recv_sem.at[sem],
            device_id={"seq": peer},
            device_id_type=MESH,
        ).start()

    partner = me + 1 - 2 * lax.rem(me, 2)
    chips = n // 2

    def pass_on(ref, chunk, sem):
        send(ref.at[chunk], ref.at[chunk], sem, partner)

    def hop(ref, step, sem, level):
        return pltpu.make_async_remote_copy(
            src_ref=ref.at[me],
            dst_ref=ref.at[me],
            send_sem=send_sem.at[sem],
            recv_sem=hop_sem.at[level, step],
            device_id={"seq": lax.rem(me + 2 * step, n)},
            device_id_type=MESH,
        )

    def spread(ref, sem, level):
        @pl.loop(1, chips)
        def _(step):
            hop(ref, step, sem, level).start()

        pass_on(ref, me, level)

    def relay(ref, sem, level):
        @pl.loop(1, chips)
        def _(step):
            hop(ref, step, sem, level).wait_recv()
            pass_on(ref, lax.rem(me - 2 * step + n, n), level)

    def settle(ref, sem, level):
        await_bytes(ref, chips - 1, send_sem.at[sem])
        await_bytes(ref, chips, recv_sem.at[level])
        await_bytes(ref, chips, send_sem.at[level])

    spread(q_ref, 2, 0)

    column = lax.broadcasted_iota(jnp.int32, (frame_count, size + EXTRA), 1)
    place = lax.broadcasted_iota(jnp.int32, (frame_count, size + EXTRA), 0)
    masks = []
    for older in range(steps):
        hidden = (place >= len_ref[older, me]) & (column == size)
        masks.append(jnp.where(hidden, MASKED, 0.0).astype(jnp.bfloat16))
    mask = jnp.concatenate(masks, axis=0)
    ones = jnp.ones((EXTRA, steps * frame_count), jnp.bfloat16)

    @pl.loop(0, heads)
    def _(head):
        k_ref[head] = mask
        vt_ref[head, size:, :] = ones

    parts = wkv_ref.shape[0] // 2
    part_heads = half // size

    def project(part, index):
        at = pl.ds(pl.multiple_of(index * tile, tile), tile)
        keyval = jnp.dot(frames_ref[index], wkv_ref[part], preferred_element_type=jnp.float32)
        return at, keyval.astype(jnp.bfloat16)

    def project_keys(part, fresh=False):
        weight_copy(part).wait()
        for index in range(tiles):
            if fresh:
                frame_copy(index).wait()
            at, keyval = project(part, index)
            for local_head in range(part_heads):
                lanes = slice(local_head * size, (local_head + 1) * size)
                k_ref[part * part_heads + local_head, at, 0:size] = keyval[:, lanes]

    project_keys(0, True)
    pl.loop(1, parts)(project_keys)

    def project_values(part):
        weight_copy(parts + part).wait()
        for index in range(tiles):
            at, keyval = project(parts + part, index)
            turned = keyval.T
            for local_head in range(part_heads):
                lanes = slice(local_head * size, (local_head + 1) * size)
                vt_ref[part * part_heads + local_head, 0:size, at] = turned[lanes]

    pl.loop(0, parts - 2)(project_values)
    relay(q_ref, 2, 0)
    pl.loop(parts - 2, parts)(project_values)
    settle(q_ref, 2, 0)

    slot_place = lax.rem(me + 1, n).astype(jnp.float32)
    distance = jnp.abs(pos_ref[...].astype(jnp.float32) - slot_place) / n
    first_row = lax.broadcasted_iota(jnp.int32, (EXTRA, tokens), 0) == 0
    query_tail = jnp.where(first_row, 1.0, 0.0).astype(jnp.bfloat16)
    token_step = lax.broadcasted_iota(jnp.int32, (1, tokens), 1) // per_step

    row = lax.broadcasted_iota(jnp.int32, (rows, tokens), 0)

    def pass_sums(turn):
        group = lax.rem(me // group_chunks + 1 + turn, groups)
        await_bytes(pair_stat, group_chunks // 2, pair_sem.at[0, turn])
        await_bytes(pair_ctx, group_chunks // 2, pair_sem.at[1, turn])

        @pl.loop(0, group_chunks // 2)
        def _(index):
            chunk = group * group_chunks + 2 * index + lax.rem(me, 2)
            slot = chunk // 2
            one, two = stat_ref[chunk], pair_stat[slot]
            top = jnp.maximum(one[0:2], two[0:2])
            one_factor = jnp.exp(one[0:2] - top)
            two_factor = jnp.exp(two[0:2] - top)
            stat = jnp.concatenate([top, one[2:4] * one_factor + two[2:4] * two_factor], axis=0)
            is_one = row + lax.rem(chunk * rows, size) < size
            context = ctx_ref[chunk].astype(jnp.float32) * jnp.where(
                is_one, one_factor[0:1], one_factor[1:2]
            ) + pair_ctx[slot].astype(jnp.float32) * jnp.where(
                is_one, two_factor[0:1], two_factor[1:2]
            )
            context = context.astype(jnp.bfloat16)

            @pl.when(chunk != me)
            def _():
                sum_stat[slot] = stat
                sum_ctx[slot] = context
                send(sum_stat.at[slot], got_stat.at[me // 2], 4, chunk)
                send(sum_ctx.at[slot], got_ctx.at[me // 2], 5, chunk)

            @pl.when(chunk == me)
            def _():
                got_stat[slot] = stat
                got_ctx[slot] = context

    @pl.loop(0, groups)
    def _(turn):
        group = lax.rem(me // group_chunks + 1 + turn, groups)
        query_rows = rows_together(q_ref, group * group_chunks, group_chunks).astype(jnp.bfloat16)
        peaks, totals, contexts = [], [], []

        def scores(local_head):
            query = jnp.concatenate(
                [query_rows[local_head * size : (local_head + 1) * size], query_tail], axis=0
            )
            return [
                jnp.dot(
                    k_ref[
                        group * group_heads + local_head,
                        pl.ds(older * frame_count, frame_count),
                        :,
                    ],
                    query[:, older * per_step :],
                    preferred_element_type=jnp.float32,
                )
                for older in range(steps)
            ]

        ready = scores(0)
        for local_head in range(group_heads):
            head = group * group_heads + local_head
            raws = ready
            if local_head + 1 < group_heads:
                ready = scores(local_head + 1)
            slope = slope_ref[head]
            peak = context = None
            for older in range(steps):
                first = older * per_step
                block = pl.ds(older * frame_count, frame_count)
                raw = raws[older]
                raw_peak = jnp.max(raw, axis=0, keepdims=True)
                weights = jnp.exp2((raw - raw_peak) * (scale * math.log2(math.e)))
                part_context = jnp.dot(
                    vt_ref[head, :, block],
                    weights.astype(jnp.bfloat16),
                    preferred_element_type=jnp.float32,
                )
                age = (token_step[:, first:] - older).astype(jnp.float32)
                part_peak = raw_peak * scale - slope * (distance[:, first:] + age)
                if peak is None:
                    peak, context = part_peak, part_context
                    continue
                top = jnp.maximum(peak[:, first:], part_peak)
                old_factor = jnp.exp(peak[:, first:] - top)
                new_factor = jnp.exp(part_peak - top)
                merged = context[:, first:] * old_factor + part_context * new_factor
                peak = jnp.concatenate([peak[:, :first], top], axis=1)
                context = jnp.concatenate([context[:, :first], merged], axis=1)
            peaks.append(peak)
            totals.append(context[size : size + 1])
            contexts.append(context[:size])
        stacked = jnp.concatenate(contexts, axis=0)
        for index in range(group_chunks):
            low, high = index * rows, (index + 1) * rows
            one, two = low // size, (high - 1) // size
            chunk = group * group_chunks + index
            ctx_ref[chunk] = stacked[low:high].astype(jnp.bfloat16)
            stat_ref[chunk] = jnp.concatenate(
                [peaks[one], peaks[two], totals[one], totals[two]], axis=0
            )

        @pl.loop(0, group_chunks // 2)
        def _(index):
            chunk = group * group_chunks + 2 * index + 1 - lax.rem(me, 2)
            for kind, (src, dst) in enumerate(((stat_ref, pair_stat), (ctx_ref, pair_ctx))):
                pltpu.make_async_remote_copy(
                    src_ref=src.at[chunk],
                    dst_ref=dst.at[chunk // 2],
                    send_sem=send_sem.at[kind],
                    recv_sem=pair_sem.at[kind, turn],
                    device_id={"seq": partner},
                    device_id_type=MESH,
                ).start()

        @pl.when(turn > 0)
        def _():
            pass_sums(turn - 1)

    pass_sums(groups - 1)
    await_bytes(got_stat, chips - 1, recv_sem.at[4])
    await_bytes(got_ctx, chips - 1, recv_sem.at[5])
    await_bytes(sum_stat, chips - 1, send_sem.at[4])
    await_bytes(sum_ctx, chips - 1, send_sem.at[5])
    await_bytes(stat_ref, chips, send_sem.at[0])
    await_bytes(ctx_ref, chips, send_sem.at[1])

    top = lax.fori_loop(
        1, chips, lambda at, best: jnp.maximum(best, got_stat[at][0:2]), got_stat[0][0:2]
    )
    is_one = row + lax.rem(me * rows, size) < size

    def add(at, state):
        total, acc = state
        stat = got_stat[at]
        factor = jnp.exp(stat[0:2] - top)
        spread = jnp.where(is_one, factor[0:1], factor[1:2])
        return total + stat[2:4] * factor, acc + got_ctx[at].astype(jnp.float32) * spread

    total, acc = lax.fori_loop(
        0,
        chips,
        add,
        (jnp.zeros((2, tokens), jnp.float32), jnp.zeros((rows, tokens), jnp.float32)),
    )
    fin_ref[me] = (acc / jnp.where(is_one, total[0:1], total[1:2])).astype(jnp.bfloat16)

    spread(fin_ref, 3, 1)
    relay(fin_ref, 3, 1)
    settle(fin_ref, 3, 1)
    context = rows_together(fin_ref, 0, n).astype(jnp.bfloat16)
    attended = jnp.dot(wout_ref[...], context, preferred_element_type=jnp.float32)
    attended = attended.astype(jnp.bfloat16)
    for step in range(steps):
        out_ref[step] = attended[:, step * per_step : (step + 1) * per_step]


def local(n, frames, dec_states, w_query, w_keyval, w_output, head_slope, lengths, positions):
    steps, frame_count, width = frames.shape
    per_step = dec_states.shape[1]
    tokens = steps * per_step
    heads = head_slope.shape[0]
    size = width // heads
    rows = w_query.shape[1]
    keys = steps * frame_count
    tile = frame_count
    part = math.gcd(width, 256)
    vmem = pl.BlockSpec(memory_space=pltpu.VMEM)
    smem = pl.BlockSpec(memory_space=pltpu.SMEM)
    hbm = pl.BlockSpec(memory_space=pl.ANY)
    out = pl.pallas_call(
        functools.partial(kernel, n),
        out_shape=jax.ShapeDtypeStruct((steps, rows, per_step), jnp.bfloat16),
        in_specs=[vmem, vmem, vmem, vmem, smem, smem, hbm, hbm],
        out_specs=vmem,
        scratch_shapes=[
            pltpu.VMEM((keys // tile, tile, width), jnp.bfloat16),
            pltpu.VMEM((2 * width // part, width, part), jnp.bfloat16),
            pltpu.VMEM((heads, keys, size + EXTRA), jnp.bfloat16),
            pltpu.VMEM((heads, size + EXTRA, keys), jnp.bfloat16),
            pltpu.VMEM((n, rows, tokens), jnp.bfloat16),
            pltpu.VMEM((n, rows, tokens), jnp.bfloat16),
            pltpu.VMEM((n, 4, tokens), jnp.float32),
            pltpu.VMEM((n // 2, rows, tokens), jnp.bfloat16),
            pltpu.VMEM((n // 2, 4, tokens), jnp.float32),
            pltpu.VMEM((n // 2, rows, tokens), jnp.bfloat16),
            pltpu.VMEM((n // 2, 4, tokens), jnp.float32),
            pltpu.VMEM((n // 2, rows, tokens), jnp.bfloat16),
            pltpu.VMEM((n // 2, 4, tokens), jnp.float32),
            pltpu.VMEM((n, rows, tokens), jnp.bfloat16),
            pltpu.SemaphoreType.DMA((keys // tile,)),
            pltpu.SemaphoreType.DMA((2 * width // part,)),
            pltpu.SemaphoreType.DMA((6,)),
            pltpu.SemaphoreType.DMA((6,)),
            pltpu.SemaphoreType.DMA((2, n // 2)),
            pltpu.SemaphoreType.DMA((2, math.gcd(heads, n))),
        ],
        compiler_params=pltpu.CompilerParams(
            collective_id=0, has_side_effects=True, vmem_limit_bytes=60 * 1024 * 1024
        ),
    )(
        dec_states.reshape(tokens, width),
        w_query.T,
        w_output.T,
        positions.reshape(1, tokens),
        head_slope,
        lengths,
        frames,
        w_keyval,
    )
    return out.transpose(0, 2, 1)


def solution(mesh):
    return jax.shard_map(
        functools.partial(local, mesh.shape["seq"]),
        mesh=mesh,
        in_specs=(
            P("grp", "seq", None),
            P(None, "grp", None),
            P(None, "seq"),
            P(),
            P(None, "seq"),
            P(),
            P("grp", None),
            P(None, "grp"),
        ),
        out_specs=P(None, "grp", "seq"),
        check_vma=False,
    )
```
